32 devices in a mesh: groups: 2 (over y), expert: 4 (over z), hidden: 4 (over x, core).
Axes of the slice: x: 2, y: 2, z: 4, core: 2. Of those that a mesh axis runs over, the one named last changes fastest.
Arguments:
- tokens: bfloat16 [512, 4096], P(('groups', 'expert'), 'hidden'), parts along dimension 0, may hold values from -6 to 6
- norm_gain: bfloat16 [4096], P('hidden'), may hold values from 0.25 to 1.75
- gate_proj: bfloat16 [64, 768, 4096], P('expert', 'hidden'), may hold values from -0.09375 to 0.09375
- up_proj: bfloat16 [64, 768, 4096], P('expert', 'hidden'), may hold values from -0.09375 to 0.09375
- down_proj: bfloat16 [64, 768, 4096], P('expert', 'hidden'), may hold values from -0.21875 to 0.21875
- expert_ids: int32 [512, 8], P(('groups', 'expert')), parts along dimension 0, may hold values from 0 to 63, as said below
- slot_ids: int32 [512, 8], P(('groups', 'expert')), parts along dimension 0, may hold values from 0 to 11, as said below
- gate_num: int32 [512, 8], P(('groups', 'expert')), parts along dimension 0, may hold values from 1 to 255
Outputs:
- layer_out: bfloat16 [512, 4096], P(('groups', 'expert'), 'hidden'), parts along dimension 0
The draws below stay inside these ranges and needn't reach their ends.
There are 2 independent parts, one for each index of `groups`. The reference program is written for one: setup_inputs(seed, part) draws one part's arguments, and reference() takes and returns one part's arrays. A program takes and returns all parts, laid end to end along the dimension named above; an argument that names none is the same for every part. Nothing has to cross between parts.
Inputs may be any that keep to these rules, and one draw needn't show every extreme that they name: `expert_ids`: each token names 8 different experts. In every aligned block of 64 tokens (the tokens of one index of the expert axis), a quarter of the experts are named by exactly 12 tokens, a quarter by 8 and the other half by 6; some expert is named by 12 tokens in every block. `slot_ids`: within an aligned block of 64 tokens, the routes that name one expert carry the slots 0 up to their count minus 1, each once.
All inputs are finite; a program needn't handle non-finite values.
Results may differ from the reference program's by a relative error of at most 0.0085.
Values may be sent and summed in bfloat16 or wider, within the bound.
A program may use at most 128 MiB of HBM per device.

```python
import jax
import jax.numpy as jnp
import numpy as np
from jax import lax

D = 4096
HID = 768
SPECIALIST_COUNT = 64
TOPK = 8
TOK_SRC = 64
CAP = 12
HID_DEV = 192
TOKENS = 256
N_EXPERT = 4
N_HIDDEN = 4


def route_layout(key):
    blocks = TOKENS // TOK_SRC
    prior_router_scores = jax.random.fold_in(key, 11)
    favoured_draw_seed, extra_draw_seed, jitter_draw_seed, sequence_draw_seed = jax.random.split(prior_router_scores, 4)
    labels = jnp.arange(SPECIALIST_COUNT, dtype=jnp.int32)
    hottest = jax.random.randint(favoured_draw_seed, (), 0, SPECIALIST_COUNT)
    specialist_extras = jax.random.randint(extra_draw_seed, (SPECIALIST_COUNT,), 0, 3) * (1 << 20)
    specialist_extras = jnp.where(labels == hottest, 3 * (1 << 20), specialist_extras)
    jitter = jax.random.randint(jitter_draw_seed, (blocks, SPECIALIST_COUNT), 0, 1 << 20)
    scores = (jitter + specialist_extras[None, :]) * SPECIALIST_COUNT + labels[None, :]
    ranked = jnp.argsort(-scores, axis=1).astype(jnp.int32)
    counts = np.array([CAP] * (SPECIALIST_COUNT // 4) + [2 * CAP // 3] * (SPECIALIST_COUNT // 4) + [CAP // 2] * (SPECIALIST_COUNT - SPECIALIST_COUNT // 2))
    starts = np.concatenate([np.zeros(1, np.int64), np.cumsum(counts)[:-1]])
    rank_of = np.repeat(np.arange(SPECIALIST_COUNT), counts)
    slot_of = np.arange(TOPK * TOK_SRC) - starts[rank_of]
    order_scores = jax.random.randint(sequence_draw_seed, (blocks, TOK_SRC), 0, 1 << 20) * TOK_SRC + jnp.arange(TOK_SRC, dtype=jnp.int32)[None, :]
    placement = jnp.argsort(order_scores, axis=1).astype(jnp.int32)
    position = jnp.arange(TOPK, dtype=jnp.int32)[None, None, :] * TOK_SRC + placement[:, :, None]
    rank_table = jnp.asarray(rank_of, dtype=jnp.int32)
    slot_table = jnp.asarray(slot_of, dtype=jnp.int32)
    ranks = rank_table[position].reshape(blocks, TOK_SRC * TOPK)
    chosen = jnp.take_along_axis(ranked, ranks, axis=1)
    slots = slot_table[position]
    return (chosen.reshape(TOKENS, TOPK).astype(jnp.int32), slots.reshape(TOKENS, TOPK).astype(jnp.int32))


def draw_expert_ids(key, part):
    return route_layout(key)[0]


def draw_slot_ids(key, part):
    return route_layout(key)[1]


def with_ends(entries, rng, low, top_value):
    longest = entries.shape.index(max(entries.shape))
    spots = []
    for shift in (0, 1):
        where = [jax.random.randint(jax.random.fold_in(rng, axis), (), 0, length) for axis, length in enumerate(entries.shape)]
        where[longest] = (where[longest] + shift) % entries.shape[longest]
        spots.append(tuple(where))
    return entries.at[spots[0]].set(low).at[spots[1]].set(top_value)


def strengthened(result, rng, source, target, blocks, factor):
    owner, partner = [(jnp.arange(result.shape[dim]) // (result.shape[dim] // blocks)).reshape([-1 if axis == dim else 1 for axis in range(result.ndim)]) for dim in (source, target)]
    chosen = jax.random.permutation(rng, blocks)[partner]
    strong = (owner == chosen) | (owner == (partner + blocks // 2) % blocks)
    return jnp.where(strong, factor * result, result)


def shard_levels(rng, dims, pieces, low, top_value):
    def one(dim, blocks):
        heights = jax.random.uniform(jax.random.fold_in(jax.random.fold_in(rng, 6), dim), (blocks,), jnp.float32, low / len(pieces), top_value / len(pieces))
        return jnp.repeat(jnp.exp(heights), dims[dim] // blocks).reshape((-1,) + (1,) * (len(dims) - dim - 1))

    level = one(*pieces[0])
    for cut in pieces[1:]:
        level = level * one(*cut)
    return level


def normal_values(rng, dims, deviation, limit, cuts=(), held_as=jnp.bfloat16):
    entries = jax.random.normal(rng, dims, jnp.float32) * deviation
    if len(cuts) > 0:
        entries = shard_levels(rng, dims, cuts, -0.22, 0.18) * entries
    return jnp.clip(entries, min=-limit, max=limit).astype(held_as)


def bell_draw_with(rng, dims, scale, reach, cuts, heavy, kind=jnp.bfloat16):
    drawn = scale * jax.random.normal(rng, dims, jnp.float32)
    if cuts:
        drawn = drawn * shard_levels(rng, dims, cuts, -0.22, 0.18)
    return jnp.clip(strengthened(drawn, jax.random.fold_in(rng, 3), *heavy), -reach, reach).astype(kind)


def setup_inputs(seed: int = 0, part: int = 0) -> dict:
    streams_of = jax.random.split(jax.random.key(seed), 9)
    part_splits = jax.random.split(jax.random.fold_in(streams_of[8], part), 9)
    return {
        "tokens": bell_draw_with(part_splits[0], (TOKENS, D), 1.0, 6.0, ((0, 4), (1, 4)), (1, 0, 4, 2.0)),
        "norm_gain": jnp.clip(1.0 + 0.15 * jax.random.normal(streams_of[1], (D,), jnp.float32), 0.25, 1.75).astype(jnp.bfloat16),
        "gate_proj": normal_values(streams_of[2], (SPECIALIST_COUNT, HID, D), D ** -0.5, 0.09375, ((0, 4), (1, 4))),
        "up_proj": normal_values(streams_of[3], (SPECIALIST_COUNT, HID, D), D ** -0.5, 0.09375, ((0, 4), (1, 4))),
        "down_proj": normal_values(streams_of[4], (SPECIALIST_COUNT, HID, D), HID ** -0.5, 0.21875, ((0, 4), (1, 4))),
        "expert_ids": draw_expert_ids(jax.random.fold_in(jax.random.fold_in(streams_of[8], part), 71), part),
        "slot_ids": draw_slot_ids(jax.random.fold_in(jax.random.fold_in(streams_of[8], part), 71), part),
        "gate_num": with_ends(jax.random.randint(part_splits[7], (TOKENS, TOPK), 1, 256), jax.random.fold_in(part_splits[7], 1), 1, 255).astype(jnp.int32),
    }


gate_scale = 1.0 / 1024.0

def expert_block(operands):
    inputs, gate_weight, up_weight, down_weight = operands
    flat_rows = inputs.reshape(-1, D)
    gate_act = jnp.dot(flat_rows, gate_weight.T, preferred_element_type=jnp.float32)
    up_act = jnp.dot(flat_rows, up_weight.T, preferred_element_type=jnp.float32)
    activated = (jax.nn.silu(gate_act) * up_act).astype(jnp.bfloat16)
    split_act = activated.reshape(-1, N_HIDDEN, HID_DEV).astype(jnp.float32)
    split_down = down_weight.reshape(N_HIDDEN, HID_DEV, D).astype(jnp.float32)
    partials = jnp.einsum('rjh,jhd->jrd', split_act, split_down).astype(jnp.bfloat16)
    partials = lax.optimization_barrier(partials)
    return lax.optimization_barrier(jnp.sum(partials.astype(jnp.float32), axis=0)).reshape(N_EXPERT, CAP, D)

def reference(tokens, norm_gain, gate_proj, up_proj, down_proj, expert_ids, slot_ids, gate_num):
    features = tokens.astype(jnp.float32)
    squares = lax.optimization_barrier(jnp.sum(features * features, axis=1))
    scale = lax.rsqrt(squares / D + 0.5)
    normed = (features * scale[:, None] * norm_gain.astype(jnp.float32)[None, :]).astype(jnp.bfloat16)
    source = (jnp.arange(TOKENS) // TOK_SRC).astype(jnp.int32)
    buffer = jnp.zeros((SPECIALIST_COUNT, N_EXPERT, CAP, D), jnp.bfloat16)
    spread_rows = jnp.broadcast_to(normed[:, None, :], (TOKENS, TOPK, D))
    buffer = buffer.at[expert_ids, source[:, None], slot_ids].set(spread_rows)
    expert_out = lax.map(expert_block, (buffer, gate_proj, up_proj, down_proj))
    picked = expert_out[expert_ids, source[:, None], slot_ids]
    gates = gate_num.astype(jnp.float32) * gate_scale
    return lax.optimization_barrier(jnp.sum(picked * gates[:, :, None], axis=1)).astype(jnp.bfloat16)
```

```python
import functools

import jax
import jax.numpy as jnp
from jax import lax
from jax.experimental import pallas as pl
from jax.experimental.pallas import tpu as pltpu
from jax.sharding import PartitionSpec as P

D = 4096
SPECIALIST_COUNT = 64
CAP = 12


gate_scale = 1.0 / 1024.0


def route_tables(expert_ids, slot_ids, gate_num):
    slot_index = expert_ids * CAP + slot_ids
    columns = lax.broadcasted_iota(jnp.int32, (1, 1, SPECIALIST_COUNT * CAP), 2)
    matches = slot_index[:, :, None] == columns
    placing = jnp.any(matches, axis=1).astype(jnp.bfloat16)
    scaled = gate_num.astype(jnp.float32) * gate_scale
    weights = jnp.sum(jnp.where(matches, scaled[:, :, None], 0.0), axis=1).astype(jnp.bfloat16)
    return (placing, weights)


def normalize(features, gain, total_squares):
    scale = lax.rsqrt(total_squares / D + 0.5)
    return (
        features.astype(jnp.float32) * scale[:, None] * gain.astype(jnp.float32)[None, :]
    ).astype(jnp.bfloat16)


def place_rows(placing, normed, sources):
    outgoing = lax.dot_general(
        placing, normed, (((0,), (0,)), ((), ())), preferred_element_type=jnp.float32
    )
    return outgoing.astype(jnp.bfloat16).reshape(sources, -1, CAP, normed.shape[1])


def on_device(tokens, norm_gain, gate_proj, up_proj, down_proj, expert_ids, slot_ids, gate_num):
    sources = lax.axis_size("expert")
    placing, weights = route_tables(expert_ids, slot_ids, gate_num)
    local_squares = jnp.sum(jnp.square(tokens.astype(jnp.float32)), axis=1)
    squares = lax.psum(local_squares, "hidden")
    normed = normalize(tokens, norm_gain, squares)
    outgoing = place_rows(placing, normed, sources)
    received = lax.all_to_all(outgoing, "expert", split_axis=0, concat_axis=2, tiled=True)[0]
    block_cols = lax.all_gather(received, "hidden", axis=2, tiled=True)
    gate_more = jnp.einsum(
        "ehd,erd->ehr", gate_proj, block_cols, preferred_element_type=jnp.float32
    )
    up_more = jnp.einsum("ehd,erd->ehr", up_proj, block_cols, preferred_element_type=jnp.float32)
    activated = (jax.nn.silu(gate_more) * up_more).astype(jnp.bfloat16)
    partial_value = jnp.einsum(
        "ehr,ehd->erd", activated, down_proj, preferred_element_type=jnp.float32
    ).astype(jnp.bfloat16)
    returned = lax.all_to_all(
        partial_value[None], "expert", split_axis=2, concat_axis=0, tiled=True
    )
    returned = returned.reshape(-1, returned.shape[-1])
    partial_out = jnp.dot(weights, returned, preferred_element_type=jnp.float32)
    return lax.psum_scatter(partial_out, "hidden", scatter_dimension=1, tiled=True).astype(
        jnp.bfloat16
    )


MESH = pl.DeviceIdType.MESH
PACK = 1024


def fused_kernel(
    dims, tok_ref, gain_ref, route_ref, gate_ref, up_ref, down_ref, out_ref,
    wbuf, xall, xn, gbuf, rtab, wcol, abuf, pbuf, sibr, r1, r2m, r2p, r3t, r3b, r4, r5m, r5p, tbuf,
    wsem, dsem, lsem, ssem, rsem,
):
    rows, feat, per, units, experts, slots = dims
    half = rows // 2
    zn, hn = 4, 4
    d = feat * hn
    group = per * units
    z = lax.axis_index("expert")
    h = lax.axis_index("hidden")
    g = lax.axis_index("groups")
    x, c = h // 2, h % 2
    zp, zm, z2 = (z + 1) % zn, (z + 3) % zn, (z + 2) % zn
    hx = (1 - x) * 2 + c
    hs = x * 2 + (1 - c)
    hd = (1 - x) * 2 + (1 - c)
    XP, SIB = (g, z, hx), (g, z, hs)
    ZP, ZM, Z2 = (g, zp, h), (g, zm, h), (g, z2, h)

    def weight_copies(p):
        out = []
        for i in range(per):
            for j, ref in enumerate((gate_ref, up_ref)):
                out.append(pltpu.make_async_copy(
                    ref.at[per * p + i],
                    wbuf.at[p, pl.ds(j * group + i * units, units), :],
                    wsem.at[p, per * j + i],
                ))
        return out

    def down_copies(s):
        return [
            pltpu.make_async_copy(
                down_ref.at[2 * per * s + i], wbuf.at[s, pl.ds(i * units, units), :], dsem.at[s, i]
            )
            for i in range(2 * per)
        ]

    for p in range(slots):
        for copy in weight_copies(p):
            copy.start()

    barrier = pltpu.get_barrier_semaphore()
    for peer in (XP, SIB, ZP, ZM, Z2):
        pl.semaphore_signal(barrier, inc=1, device_id=peer, device_id_type=MESH)
    pl.semaphore_wait(barrier, 5)

    sends = []

    def send(index, src, dst, peer):
        copy = pltpu.make_async_remote_copy(
            src_ref=src, dst_ref=dst, send_sem=ssem.at[index], recv_sem=rsem.at[index],
            device_id=peer, device_id_type=MESH,
        )
        copy.start()
        sends.append(copy)

    def arrived(index, dst):
        pltpu.make_async_remote_copy(
            src_ref=dst, dst_ref=dst, send_sem=ssem.at[index], recv_sem=rsem.at[index],
            device_id=SIB, device_id_type=MESH,
        ).wait_recv()

    def blk(hh, zz):
        return xall.at[hh, pl.ds(pl.multiple_of(zz * rows, rows), rows), :]

    def blk_half(hh, zz, which):
        return xall.at[hh, pl.ds(pl.multiple_of(zz * rows + which * half, half), half), :]

    send(0, tok_ref, blk(h, z), XP)
    send(1, tok_ref, blk(h, z), ZP)
    send(2, tok_ref, blk(h, z), ZM)
    send(3, gain_ref, gbuf.at[h], XP)
    send(4, route_ref, rtab.at[z], ZP)
    send(5, route_ref, rtab.at[z], ZM)
    send(6, route_ref, rtab.at[z], Z2)
    send(7, gain_ref, gbuf.at[h], SIB)
    send(8, tok_ref, blk(h, z), SIB)
    local = [
        pltpu.make_async_copy(tok_ref, blk(h, z), lsem.at[0]),
        pltpu.make_async_copy(gain_ref, gbuf.at[h], lsem.at[1]),
        pltpu.make_async_copy(route_ref, rtab.at[z], lsem.at[2]),
    ]
    for copy in local:
        copy.start()
    arrived(1, blk(h, zm))
    send(9, blk_half(h, zm, 0), blk_half(h, zm, 0), ZP)
    arrived(2, blk(h, zp))
    send(10, blk_half(h, zp, 1), blk_half(h, zp, 1), ZM)
    arrived(0, blk(hx, z))
    send(11, blk(hx, z), blk(hx, z), ZP)
    send(12, blk(hx, z), blk(hx, z), ZM)
    send(13, blk(h, zm), blk(h, zm), SIB)
    send(14, blk(h, zp), blk(h, zp), SIB)
    send(15, blk(hx, z), blk(hx, z), SIB)
    arrived(3, gbuf.at[hx])
    send(16, gbuf.at[hx], gbuf.at[hx], SIB)
    arrived(9, blk_half(h, z2, 0))
    arrived(10, blk_half(h, z2, 1))
    send(17, blk(h, z2), blk(h, z2), XP)
    send(18, blk(h, z2), blk(h, z2), SIB)

    for copy in local:
        copy.wait()
    arrived(4, rtab.at[zm])
    arrived(5, rtab.at[zp])
    arrived(6, rtab.at[z2])
    lanes = wcol.shape[1]
    named = lax.broadcasted_iota(jnp.int32, (lanes, rows), 0) + z * experts
    for zb in range(zn):
        total = jnp.zeros((lanes, rows), jnp.int32)
        for k in range(rtab.shape[1]):
            row = rtab[zb, k : k + 1, :]
            total = total + jnp.where((row >> 10) == named, row & (PACK - 1), 0)
        wcol[zb * rows : (zb + 1) * rows, :] = (total.astype(jnp.float32) * gate_scale).T

    arrived(11, blk(hx, zm))
    send(19, blk(hx, zm), blk(hx, zm), SIB)
    arrived(12, blk(hx, zp))
    send(20, blk(hx, zp), blk(hx, zp), SIB)
    arrived(17, blk(hx, z2))
    send(21, blk(hx, z2), blk(hx, z2), SIB)
    arrived(7, gbuf.at[hs])
    arrived(16, gbuf.at[hd])
    arrived(8, blk(hs, z))
    arrived(13, blk(hs, zm))
    arrived(14, blk(hs, zp))
    arrived(15, blk(hd, z))
    arrived(18, blk(hs, z2))
    arrived(19, blk(hd, zm))
    arrived(20, blk(hd, zp))
    arrived(21, blk(hd, z2))

    def normal(i, carry):
        at = pl.ds(pl.multiple_of(i * half, half), half)
        squares = jnp.zeros((half, 1), jnp.float32)
        for hh in range(hn):
            piece = xall[hh, at, :].astype(jnp.float32)
            squares = squares + jnp.sum(piece * piece, axis=1, keepdims=True)
        scale = lax.rsqrt(squares / d + 0.5)
        for hh in range(hn):
            piece = xall[hh, at, :].astype(jnp.float32)
            xn[at, hh * feat : (hh + 1) * feat] = (piece * scale * gbuf[hh]).astype(jnp.bfloat16)
        return carry

    lax.fori_loop(0, 2 * zn, normal, 0)

    def expert_pair(p):
        for copy in weight_copies(p):
            copy.wait()
        both = lax.dot_general(
            xn[...], wbuf[p], (((1,), (1,)), ((), ())), preferred_element_type=jnp.float32
        )
        gate, up = both[:, :group], both[:, group:]
        table = wcol[...]
        lane = lax.broadcasted_iota(jnp.int32, table.shape, 1)
        wide = lax.broadcasted_iota(jnp.int32, gate.shape, 1)
        weight = jnp.zeros(gate.shape, jnp.float32)
        for i in range(per):
            col = jnp.sum(jnp.where(lane == per * p + i, table, 0.0), axis=1, keepdims=True)
            weight = jnp.where((wide >= i * units) & (wide < (i + 1) * units), col, weight)
        act = gate / (1.0 + jnp.exp(-gate)) * up
        act = jnp.where(weight > 0.0, act * weight, 0.0)
        abuf[:, pl.ds(pl.multiple_of(p * group, 128), group)] = act.astype(jnp.bfloat16)

    def first(p, carry):
        expert_pair(p)
        for copy in down_copies(p):
            copy.start()
        return carry

    def second(p, carry):
        expert_pair(p)
        return carry

    lax.fori_loop(0, slots // 2, first, 0)
    lax.fori_loop(slots // 2, slots, second, 0)
    for s in range(slots // 2):
        for copy in down_copies(s):
            copy.wait()

    tile = 256

    def down(hh, place):
        def body(i, carry):
            cols = pl.ds(pl.multiple_of(hh * feat + i * tile, tile), tile)
            dense = wbuf[: slots // 2, :, cols].reshape(-1, tile)
            value = jnp.dot(abuf[...], dense, preferred_element_type=jnp.float32)
            pbuf[place, :, pl.ds(pl.multiple_of(i * tile, tile), tile)] = value.astype(jnp.bfloat16)
            return carry

        lax.fori_loop(0, feat // tile, body, 0)

    f32, b16 = jnp.float32, jnp.bfloat16

    def join(place, other):
        def body(i, carry):
            at = pl.ds(pl.multiple_of(i * rows, rows), rows)
            value = pbuf[place, at, :].astype(f32) + sibr[other, at, :].astype(f32)
            pbuf[place, at, :] = value.astype(b16)
            return carry

        lax.fori_loop(0, zn, body, 0)

    def at_rows(zz):
        return pl.ds(pl.multiple_of(zz * rows, rows), rows)

    def at_half(zz, which):
        return pl.ds(pl.multiple_of(zz * rows + which * half, half), half)

    down(hd, 0)
    send(22, pbuf.at[0], sibr.at[0], SIB)
    down(hx, 1)
    arrived(22, sibr.at[0])
    join(1, 0)
    send(23, pbuf.at[1, at_rows(z2), :], r1, XP)
    send(24, pbuf.at[1, at_rows(zp), :], r2m, ZP)
    send(25, pbuf.at[1, at_rows(zm), :], r2p, ZM)
    down(hs, 2)
    send(26, pbuf.at[2], sibr.at[1], SIB)
    down(h, 3)
    arrived(26, sibr.at[1])
    join(3, 1)
    arrived(23, r1)
    tbuf[0] = (pbuf[3, at_rows(z2), :].astype(f32) + r1[...].astype(f32)).astype(b16)
    send(27, tbuf.at[0, pl.ds(0, half), :], r3t, ZP)
    send(28, tbuf.at[0, pl.ds(half, half), :], r3b, ZM)
    send(29, pbuf.at[3, at_half(zp, 1), :], r5m.at[pl.ds(half, half), :], ZP)
    send(30, pbuf.at[3, at_half(zm, 0), :], r5p.at[pl.ds(0, half), :], ZM)
    arrived(24, r2m)
    arrived(25, r2p)
    tbuf[1] = (pbuf[1, at_rows(z), :].astype(f32) + r2m[...].astype(f32) + r2p[...].astype(f32)).astype(b16)
    send(31, tbuf.at[1], r4, XP)
    arrived(27, r3t)
    tbuf[2, 0:half, :] = (pbuf[3, at_half(zp, 0), :].astype(f32) + r3t[...].astype(f32)).astype(b16)
    send(32, tbuf.at[2, pl.ds(0, half), :], r5m.at[pl.ds(0, half), :], ZP)
    arrived(28, r3b)
    tbuf[2, half:rows, :] = (pbuf[3, at_half(zm, 1), :].astype(f32) + r3b[...].astype(f32)).astype(b16)
    send(33, tbuf.at[2, pl.ds(half, half), :], r5p.at[pl.ds(half, half), :], ZM)
    arrived(31, r4)
    arrived(29, r5m.at[pl.ds(half, half), :])
    arrived(30, r5p.at[pl.ds(0, half), :])
    arrived(32, r5m.at[pl.ds(0, half), :])
    arrived(33, r5p.at[pl.ds(half, half), :])
    out_ref[...] = (
        pbuf[3, at_rows(z), :].astype(f32) + r4[...].astype(f32) + r5m[...].astype(f32) + r5p[...].astype(f32)
    ).astype(b16)
    for copy in sends:
        copy.wait_send()


def fused_on_device(tokens, norm_gain, gate_proj, up_proj, down_proj, expert_ids, slot_ids, gate_num):
    rows, feat = tokens.shape
    experts, units, d = gate_proj.shape
    zn, per = lax.axis_size("expert"), 2
    slots = experts // per
    total = rows * zn
    packed = (expert_ids * PACK + gate_num).T
    bf = jnp.bfloat16
    dims = (rows, feat, per, units, experts, slots)
    vm = pl.BlockSpec(memory_space=pltpu.VMEM)
    anywhere = pl.BlockSpec(memory_space=pl.ANY)
    block = pltpu.VMEM((rows, feat), bf)
    small = pltpu.VMEM((rows // 2, feat), bf)
    dma = pltpu.SemaphoreType.DMA
    return pl.pallas_call(
        functools.partial(fused_kernel, dims),
        out_shape=jax.ShapeDtypeStruct((rows, feat), bf),
        in_specs=[vm, vm, vm, anywhere, anywhere, anywhere],
        out_specs=vm,
        scratch_shapes=[
            pltpu.VMEM((slots, 2 * per * units, d), bf),
            pltpu.VMEM((d // feat, total, feat), bf),
            pltpu.VMEM((total, d), bf),
            pltpu.VMEM((d // feat, 1, feat), jnp.float32),
            pltpu.VMEM((zn,) + packed.shape, jnp.int32),
            pltpu.VMEM((total, 128), jnp.float32),
            pltpu.VMEM((total, experts * units), bf),
            pltpu.VMEM((4, total, feat), bf),
            pltpu.VMEM((2, total, feat), bf),
            block, block, block, small, small, block, block, block,
            pltpu.VMEM((3, rows, feat), bf),
            dma((slots, 2 * per)),
            dma((slots // 2, 2 * per)),
            dma((3,)),
            dma((34,)),
            dma((34,)),
        ],
        compiler_params=pltpu.CompilerParams(
            collective_id=0, has_side_effects=True, vmem_limit_bytes=67043328
        ),
    )(tokens, norm_gain.astype(jnp.float32)[None, :], packed, gate_proj, up_proj, down_proj)


def solution(mesh):
    square = mesh.shape["expert"] == 4 and mesh.shape["hidden"] == 4
    placed = (
        P(("groups", "expert"), "hidden"),
        P("hidden"),
        P("expert", "hidden", None),
        P("expert", "hidden", None),
        P("expert", "hidden", None),
        P(("groups", "expert"), None),
        P(("groups", "expert"), None),
        P(("groups", "expert"), None),
    )
    return jax.shard_map(
        fused_on_device if square else on_device,
        mesh=mesh,
        in_specs=placed,
        out_specs=P(("groups", "expert"), "hidden"),
        check_vma=False,
    )
```

```python
import functools

import jax
import jax.numpy as jnp
from jax import lax
from jax.experimental import pallas as pl
from jax.experimental.pallas import tpu as pltpu
from jax.sharding import PartitionSpec as P

D = 4096
SPECIALIST_COUNT = 64
CAP = 12


gate_scale = 1.0 / 1024.0


def route_tables(expert_ids, slot_ids, gate_num):
    slot_index = expert_ids * CAP + slot_ids
    columns = lax.broadcasted_iota(jnp.int32, (1, 1, SPECIALIST_COUNT * CAP), 2)
    matches = slot_index[:, :, None] == columns
    placing = jnp.any(matches, axis=1).astype(jnp.bfloat16)
    scaled = gate_num.astype(jnp.float32) * gate_scale
    weights = jnp.sum(jnp.where(matches, scaled[:, :, None], 0.0), axis=1).astype(jnp.bfloat16)
    return (placing, weights)


def normalize(features, gain, total_squares):
    scale = lax.rsqrt(total_squares / D + 0.5)
    return (
        features.astype(jnp.float32) * scale[:, None] * gain.astype(jnp.float32)[None, :]
    ).astype(jnp.bfloat16)


def place_rows(placing, normed, sources):
    outgoing = lax.dot_general(
        placing, normed, (((0,), (0,)), ((), ())), preferred_element_type=jnp.float32
    )
    return outgoing.astype(jnp.bfloat16).reshape(sources, -1, CAP, normed.shape[1])


def on_device(tokens, norm_gain, gate_proj, up_proj, down_proj, expert_ids, slot_ids, gate_num):
    sources = lax.axis_size("expert")
    placing, weights = route_tables(expert_ids, slot_ids, gate_num)
    local_squares = jnp.sum(jnp.square(tokens.astype(jnp.float32)), axis=1)
    squares = lax.psum(local_squares, "hidden")
    normed = normalize(tokens, norm_gain, squares)
    outgoing = place_rows(placing, normed, sources)
    received = lax.all_to_all(outgoing, "expert", split_axis=0, concat_axis=2, tiled=True)[0]
    block_cols = lax.all_gather(received, "hidden", axis=2, tiled=True)
    gate_more = jnp.einsum(
        "ehd,erd->ehr", gate_proj, block_cols, preferred_element_type=jnp.float32
    )
    up_more = jnp.einsum("ehd,erd->ehr", up_proj, block_cols, preferred_element_type=jnp.float32)
    activated = (jax.nn.silu(gate_more) * up_more).astype(jnp.bfloat16)
    partial_value = jnp.einsum(
        "ehr,ehd->erd", activated, down_proj, preferred_element_type=jnp.float32
    ).astype(jnp.bfloat16)
    returned = lax.all_to_all(
        partial_value[None], "expert", split_axis=2, concat_axis=0, tiled=True
    )
    returned = returned.reshape(-1, returned.shape[-1])
    partial_out = jnp.dot(weights, returned, preferred_element_type=jnp.float32)
    return lax.psum_scatter(partial_out, "hidden", scatter_dimension=1, tiled=True).astype(
        jnp.bfloat16
    )


MESH = pl.DeviceIdType.MESH


def fused_kernel(
    dims, tok_ref, gain_ref, ids_ref, num_ref, gate_ref, up_ref, down_ref, out_ref,
    wbuf, xall, xn, gbuf, rtab, wcol, abuf, pbuf, sibr, rx, ob, qb, ib, tbuf,
    wsem, dsem, lsem, ssem, rsem,
):
    rows, feat, per, units, experts, slots = dims
    half = rows // 2
    zn, hn = 4, 4
    near = 2 * rows
    d = feat * hn
    topk = ids_ref.shape[0]
    group = per * units
    z = lax.axis_index("expert")
    h = lax.axis_index("hidden")
    g = lax.axis_index("groups")
    x, c = h // 2, h % 2
    z1, z3 = z + 1 - 2 * (z % 2), 3 - z
    z2 = (z + 2) % 4
    is_inner = (z == 1) | (z == 2)
    is_outer = (z == 0) | (z == 3)
    inner = (z % 2 + z // 2) % 2
    hx = (1 - x) * 2 + c
    hs = x * 2 + (1 - c)
    hd = (1 - x) * 2 + (1 - c)
    XP, SIB, NEAR, ACROSS = (g, z, hx), (g, z, hs), (g, z1, h), (g, z3, h)
    f32, b16 = jnp.float32, jnp.bfloat16

    def weight_copies(p):
        out = []
        for i in range(per):
            for j, ref in enumerate((gate_ref, up_ref)):
                out.append(pltpu.make_async_copy(
                    ref.at[per * p + i],
                    wbuf.at[p, pl.ds(j * group + i * units, units), :],
                    wsem.at[p, per * j + i],
                ))
        return out

    def down_copies(s):
        return [
            pltpu.make_async_copy(
                down_ref.at[2 * per * s + i], wbuf.at[s, pl.ds(i * units, units), :], dsem.at[s, i]
            )
            for i in range(2 * per)
        ]

    barrier = pltpu.get_barrier_semaphore()
    for peer in (XP, SIB, NEAR):
        pl.semaphore_signal(barrier, inc=1, device_id=peer, device_id_type=MESH)

    @pl.when(is_inner)
    def _():
        pl.semaphore_signal(barrier, inc=1, device_id=ACROSS, device_id_type=MESH)

    pl.semaphore_wait(barrier, 3 + inner)

    numbers, sends = {}, []

    def number(key):
        return numbers.setdefault(key, len(numbers))

    def make(key, tail, src, dst, peer):
        return pltpu.make_async_remote_copy(
            src_ref=src, dst_ref=dst, send_sem=ssem.at[number(key + tail)], recv_sem=rsem.at[number(key)],
            device_id=peer, device_id_type=MESH,
        )

    def send(key, src, dst, peer, when=None, tail=()):
        copy = make(key, tail, src, dst, peer)
        sends.append((copy, when))
        if when is None:
            copy.start()
        else:
            pl.when(when)(copy.start)

    def arrived(key, dst, when=None):
        copy = make(key, (), dst, dst, SIB)
        if when is None:
            copy.wait_recv()
        else:
            pl.when(when)(copy.wait_recv)

    def blk(hh, pos, which=None):
        if which is None:
            return xall.at[hh, pl.ds(pl.multiple_of(pos * rows, rows), rows), :]
        return xall.at[hh, pl.ds(pl.multiple_of(pos * rows + which * half, half), half), :]

    def tok(which):
        return tok_ref.at[pl.ds(which * half, half), :]

    for w in range(2):
        send(("z", 1, w), tok(w), blk(h, 1, w), NEAR)
        send(("z", "mid", w), tok(w), blk(h, 3, w), ACROSS, is_inner, ("own",))
        send(("x", 0, w), tok(w), blk(h, 0, w), XP)
    for name, ref, at in (("i", ids_ref, 0), ("n", num_ref, topk)):
        send((name, 1), ref, rtab.at[1, pl.ds(at, topk), :], NEAR)
        send((name, "mid"), ref, rtab.at[3, pl.ds(at, topk), :], ACROSS, is_inner, ("own",))
    send(("gx",), gain_ref, gbuf.at[h], XP)
    send(("gs",), gain_ref, gbuf.at[h], SIB)
    send(("s", 0), tok_ref, blk(h, 0), SIB)
    local = [
        pltpu.make_async_copy(tok_ref, blk(h, 0), lsem.at[0]),
        pltpu.make_async_copy(gain_ref, gbuf.at[h], lsem.at[1]),
        pltpu.make_async_copy(ids_ref, rtab.at[0, pl.ds(0, topk), :], lsem.at[2]),
        pltpu.make_async_copy(num_ref, rtab.at[0, pl.ds(topk, topk), :], lsem.at[3]),
    ]
    for copy in local:
        copy.start()

    for p in range(slots):
        for copy in weight_copies(p):
            copy.start()

    def route(pos, at):
        return rtab.at[pos, pl.ds(at, topk), :]

    place = {0: 0, 1: 1, "mid": 2 + inner, "last": 3 - inner}

    def relay(name, target, there, peer):
        pos = place[name]
        for w in range(2):
            arrived(("z", name, w), blk(h, pos, w))
            send(("z", target, w), blk(h, pos, w), blk(h, there, w), peer, is_inner, ("on", name))
            send(("x", name, w), blk(h, pos, w), blk(h, pos, w), XP)
        for kind, at in (("i", 0), ("n", topk)):
            arrived((kind, name), route(pos, at))
            send((kind, target), route(pos, at), route(there, at), peer, is_inner, ("on", name))
        send(("s", name), blk(h, pos), blk(h, pos), SIB)

    def pass_over(name):
        pos = place[name]
        for w in range(2):
            arrived(("x", name, w), blk(hx, pos, w))
        send(("t", name), blk(hx, pos), blk(hx, pos), SIB)

    def from_sibling(name):
        arrived(("s", name), blk(hs, place[name]))
        arrived(("t", name), blk(hd, place[name]))

    lanes = wcol.shape[1]
    named = lax.broadcasted_iota(jnp.int32, (lanes, rows), 0) + z * experts

    def weigh(pos):
        total = jnp.zeros((lanes, rows), jnp.int32)
        for k in range(topk):
            total = total + jnp.where(
                rtab[pos, k : k + 1, :] == named, rtab[pos, topk + k : topk + k + 1, :], 0
            )
        wcol[pos * rows : (pos + 1) * rows, :] = (total.astype(f32) * gate_scale).T

    def normal(start):
        def body(i, carry):
            at = pl.ds(pl.multiple_of(i * half + start, half), half)
            squares = jnp.zeros((half, 1), f32)
            for hh in range(hn):
                piece = xall[hh, at, :].astype(f32)
                squares = squares + jnp.sum(piece * piece, axis=1, keepdims=True)
            scale = lax.rsqrt(squares / d + 0.5)
            for hh in range(hn):
                piece = xall[hh, at, :].astype(f32)
                gain = gbuf[hh].astype(f32)
                xn[at, hh * feat : (hh + 1) * feat] = (piece * scale * gain).astype(b16)
            return carry

        lax.fori_loop(0, near // half, body, 0)

    def expert_pair(p):
        both = lax.dot_general(
            xn[...], wbuf[p], (((1,), (1,)), ((), ())), preferred_element_type=f32
        )
        gate, up = both[:, :group], both[:, group:]
        table = wcol[...]
        lane = lax.broadcasted_iota(jnp.int32, table.shape, 1)
        wide = lax.broadcasted_iota(jnp.int32, gate.shape, 1)
        weight = jnp.zeros(gate.shape, f32)
        for i in range(per):
            col = jnp.sum(jnp.where(lane == per * p + i, table, 0.0), axis=1, keepdims=True)
            weight = jnp.where((wide >= i * units) & (wide < (i + 1) * units), col, weight)
        act = gate / (1.0 + jnp.exp(-gate)) * up
        act = jnp.where(weight > 0.0, act * weight, 0.0)
        abuf[:, pl.ds(pl.multiple_of(p * group, 128), group)] = act.astype(b16)

    relay(1, "last", 2, ACROSS)
    relay("mid", "mid", 2, NEAR)
    pass_over(0)
    arrived(("gx",), gbuf.at[hx])
    send(("gt",), gbuf.at[hx], gbuf.at[hx], SIB)
    for copy in local:
        copy.wait()
    relay("last", "last", 3, NEAR)
    pass_over(1)
    pass_over("mid")
    for pos in range(zn):
        weigh(pos)
    arrived(("gs",), gbuf.at[hs])
    arrived(("gt",), gbuf.at[hd])
    from_sibling(0)
    from_sibling(1)
    normal(0)
    pass_over("last")
    from_sibling("mid")
    from_sibling("last")
    normal(near)

    def first(p, carry):
        for copy in weight_copies(p):
            copy.wait()
        expert_pair(p)
        for copy in down_copies(p):
            copy.start()
        return carry

    def second(p, carry):
        for copy in weight_copies(p):
            copy.wait()
        expert_pair(p)
        return carry

    lax.fori_loop(0, slots // 2, first, 0)
    lax.fori_loop(slots // 2, slots, second, 0)
    for s in range(slots // 2):
        for copy in down_copies(s):
            copy.wait()

    tile = 256

    def down(hh, place):
        def body(i, carry):
            cols = pl.ds(pl.multiple_of(hh * feat + i * tile, tile), tile)
            dense = wbuf[: slots // 2, :, cols].reshape(-1, tile)
            value = jnp.dot(abuf[...], dense, preferred_element_type=f32)
            pbuf[place, :, pl.ds(pl.multiple_of(i * tile, tile), tile)] = value.astype(b16)
            return carry

        lax.fori_loop(0, feat // tile, body, 0)

    def part(pos, w):
        return pl.ds(pl.multiple_of(pos * rows + w * half, half), half)

    order = [3 - inner, 2 + inner, 1, 0]
    down(hd, 0)
    send(("c", 0), pbuf.at[0], sibr.at[0], SIB)
    down(hx, 1)
    arrived(("c", 0), sibr.at[0])
    for n, pos in enumerate(order):
        for w in range(2):
            at = part(pos, w)
            pbuf[1, at, :] = (pbuf[1, at, :].astype(f32) + sibr[0, at, :].astype(f32)).astype(b16)
            send(("o", n, w), pbuf.at[1, at, :], rx.at[at, :], XP)
    down(hs, 2)
    send(("c", 1), pbuf.at[2], sibr.at[1], SIB)
    down(h, 3)
    arrived(("c", 1), sibr.at[1])

    def wide_at(w):
        return pl.ds(w * half, half)

    for n, pos in enumerate(order):
        for w in range(2):
            at = part(pos, w)
            arrived(("o", n, w), rx.at[at, :])
            value = pbuf[3, at, :].astype(f32) + sibr[1, at, :].astype(f32) + rx[at, :].astype(f32)
            pbuf[3, at, :] = value.astype(b16)
            if n < 3:
                send(("e", n, w), pbuf.at[3, at, :], ob.at[n, wide_at(w), :], NEAR, is_outer)
            if n < 2:
                arrived(("e", n, w), ob.at[n, wide_at(w), :], is_inner)

                @pl.when(is_inner)
                def _(n=n, w=w, at=at):
                    tbuf[n, wide_at(w), :] = (
                        pbuf[3, at, :].astype(f32) + ob[n, wide_at(w), :].astype(f32)
                    ).astype(b16)

                send(("q", n, w), tbuf.at[n, wide_at(w), :], qb.at[n, wide_at(w), :], ACROSS, is_inner)
    for w in range(2):
        arrived(("q", 0, w), qb.at[0, wide_at(w), :], is_inner)

        @pl.when(is_inner)
        def _(w=w):
            tbuf[2, wide_at(w), :] = (
                pbuf[3, part(1, w), :].astype(f32) + qb[0, wide_at(w), :].astype(f32)
            ).astype(b16)

        send(("b", w), tbuf.at[2, wide_at(w), :], ib.at[wide_at(w), :], NEAR, is_inner)
    for w in range(2):
        at = part(0, w)
        arrived(("e", 2, w), ob.at[2, wide_at(w), :], is_inner)
        arrived(("q", 1, w), qb.at[1, wide_at(w), :], is_inner)
        arrived(("b", w), ib.at[wide_at(w), :], is_outer)

        @pl.when(is_inner)
        def _(w=w, at=at):
            out_ref[wide_at(w), :] = (
                pbuf[3, at, :].astype(f32) + ob[2, wide_at(w), :].astype(f32) + qb[1, wide_at(w), :].astype(f32)
            ).astype(b16)

        @pl.when(is_outer)
        def _(w=w, at=at):
            out_ref[wide_at(w), :] = (pbuf[3, at, :].astype(f32) + ib[wide_at(w), :].astype(f32)).astype(b16)

    for copy, when in sends:
        if when is None:
            copy.wait_send()
        else:
            pl.when(when)(copy.wait_send)


def fused_on_device(tokens, norm_gain, gate_proj, up_proj, down_proj, expert_ids, slot_ids, gate_num):
    rows, feat = tokens.shape
    experts, units, d = gate_proj.shape
    zn, per = lax.axis_size("expert"), 2
    slots = experts // per
    total = rows * zn
    bf = jnp.bfloat16
    dims = (rows, feat, per, units, experts, slots)
    vm = pl.BlockSpec(memory_space=pltpu.VMEM)
    anywhere = pl.BlockSpec(memory_space=pl.ANY)
    dma = pltpu.SemaphoreType.DMA
    return pl.pallas_call(
        functools.partial(fused_kernel, dims),
        out_shape=jax.ShapeDtypeStruct((rows, feat), bf),
        in_specs=[vm, vm, vm, vm, anywhere, anywhere, anywhere],
        out_specs=vm,
        scratch_shapes=[
            pltpu.VMEM((slots, 2 * per * units, d), bf),
            pltpu.VMEM((d // feat, total, feat), bf),
            pltpu.VMEM((total, d), bf),
            pltpu.VMEM((d // feat, 1, feat), norm_gain.dtype),
            pltpu.VMEM((zn, 2 * expert_ids.shape[1], rows), jnp.int32),
            pltpu.VMEM((total, 128), jnp.float32),
            pltpu.VMEM((total, experts * units), bf),
            pltpu.VMEM((4, total, feat), bf),
            pltpu.VMEM((2, total, feat), bf),
            pltpu.VMEM((total, feat), bf),
            pltpu.VMEM((3, rows, feat), bf),
            pltpu.VMEM((2, rows, feat), bf),
            pltpu.VMEM((rows, feat), bf),
            pltpu.VMEM((3, rows, feat), bf),
            dma((slots, 2 * per)),
            dma((slots // 2, 2 * per)),
            dma((4,)),
            dma((96,)),
            dma((96,)),
        ],
        compiler_params=pltpu.CompilerParams(
            collective_id=0, has_side_effects=True, vmem_limit_bytes=67043328
        ),
    )(tokens, norm_gain[None, :], expert_ids.T, gate_num.T, gate_proj, up_proj, down_proj)


def solution(mesh):
    square = mesh.shape["expert"] == 4 and mesh.shape["hidden"] == 4
    placed = (
        P(("groups", "expert"), "hidden"),
        P("hidden"),
        P("expert", "hidden", None),
        P("expert", "hidden", None),
        P("expert", "hidden", None),
        P(("groups", "expert"), None),
        P(("groups", "expert"), None),
        P(("groups", "expert"), None),
    )
    return jax.shard_map(
        fused_on_device if square else on_device,
        mesh=mesh,
        in_specs=placed,
        out_specs=P(("groups", "expert"), "hidden"),
        check_vma=False,
    )
```
